16 devices in a mesh: ep: 16 (over z, y, x, core).
Axes of the slice: x: 2, y: 2, z: 2, core: 2. Of those that a mesh axis runs over, the one named last changes fastest.
Arguments:
- hidden: bfloat16 [32768, 1024], P('ep')
- grad_out: bfloat16 [32768, 1024], P('ep')
- w_router: bfloat16 [1024, 32], replicated
- b_router: float32 [32], replicated
- expert_ids: int32 [32768, 8], P('ep')
- slot_ids: int32 [32768, 8], P('ep')
- w_gate_up: bfloat16 [32, 1024, 1024], P('ep')
- b_gate_up: float32 [32, 1024], P('ep')
- w_down: bfloat16 [32, 512, 1024], P('ep')
- b_down: float32 [32, 1024], P('ep')
Outputs:
- output 1: bfloat16 [32768, 1024], P('ep')
- output 2: bfloat16 [32768, 1024], P('ep')
- output 3: float32 [1024, 32], replicated
- output 4: float32 [32], replicated
- output 5: float32 [32, 1024, 1024], P('ep')
- output 6: float32 [32, 1024], P('ep')
- output 7: float32 [32, 512, 1024], P('ep')
- output 8: float32 [32, 1024], P('ep')
All inputs are finite; a program needn't handle non-finite values.
Results may differ from the reference program's by a relative error of at most 0.0060219.
Values are sent between devices in bfloat16 or wider.
A program may use at most 1 GiB of HBM per device.

```python
import jax
import jax.numpy as jnp
from jax import lax

D_MODEL = 1024
FF_EXPERT = 512
EXPERTS = 32
TOP_K = 8
TOKENS_DEV = 2048
EP_DEVICES = 16

TOKENS = EP_DEVICES * TOKENS_DEV
CAPACITY = (3 * TOKENS_DEV * TOP_K + 2 * EXPERTS - 1) // (2 * EXPERTS)
ROWS_EXPERT = EP_DEVICES * CAPACITY
SWIGLU_LIMIT = 7.0
SWIGLU_ALPHA = 1.702


def draw_routing(key):
    key_bias, key_dev = jax.random.split(key)
    expert_bias = jax.random.randint(key_bias, (EXPERTS,), 0, 512)
    expert_range = jnp.arange(EXPERTS, dtype=jnp.int32)
    copies = TOKENS_DEV * TOP_K

    def one_device(dev_key):
        key_noise, key_hot, key_pick, key_prio = jax.random.split(dev_key, 4)
        noise_int = jax.random.randint(key_noise, (TOKENS_DEV, EXPERTS), 0, 1024)
        hot_expert = jax.random.randint(key_hot, (), 0, EXPERTS)
        forced = jax.random.permutation(key_pick, TOKENS_DEV) < 2 * CAPACITY
        hot_bonus = jnp.where(forced[:, None] & (expert_range[None, :] == hot_expert), 4096, 0)
        scores = (noise_int + expert_bias[None, :] + hot_bonus) * EXPERTS + expert_range[None, :]
        choice = lax.top_k(scores, TOP_K)[1].astype(jnp.int32)
        flat_ids = choice.reshape(-1)
        priority = jax.random.permutation(key_prio, copies)
        sort_order = jnp.argsort(flat_ids * copies + priority)
        counts = jnp.bincount(flat_ids, length=EXPERTS)
        starts = jnp.cumsum(counts) - counts
        rank_sorted = (jnp.arange(copies, dtype=jnp.int32) - starts[flat_ids[sort_order]]).astype(jnp.int32)
        slot_rank = jnp.zeros((copies,), jnp.int32).at[sort_order].set(rank_sorted)
        slot_ids = jnp.where(slot_rank < CAPACITY, slot_rank, -1).reshape(TOKENS_DEV, TOP_K)
        return choice, slot_ids

    choice, slot_ids = jax.vmap(one_device)(jax.random.split(key_dev, EP_DEVICES))
    return choice.reshape(TOKENS, TOP_K), slot_ids.reshape(TOKENS, TOP_K).astype(jnp.int32)


def setup_inputs(seed: int = 0) -> dict:
    key_list = jax.random.split(jax.random.key(seed), 9)
    hidden = jax.random.normal(key_list[0], (TOKENS, D_MODEL), jnp.float32).astype(jnp.bfloat16)
    grad_out = jax.random.normal(key_list[1], (TOKENS, D_MODEL), jnp.float32).astype(jnp.bfloat16)
    w_router = (2.0 * D_MODEL ** -0.5 * jax.random.normal(key_list[2], (D_MODEL, EXPERTS), jnp.float32)).astype(jnp.bfloat16)
    b_router = jax.random.normal(key_list[3], (EXPERTS,), jnp.float32)
    expert_ids, slot_ids = draw_routing(key_list[4])
    w_gate_up = (3.0 * D_MODEL ** -0.5 * jax.random.normal(key_list[5], (EXPERTS, D_MODEL, 2 * FF_EXPERT), jnp.float32)).astype(jnp.bfloat16)
    b_gate_up = jax.random.normal(key_list[6], (EXPERTS, 2 * FF_EXPERT), jnp.float32)
    w_down = (0.15 * FF_EXPERT ** -0.5 * jax.random.normal(key_list[7], (EXPERTS, FF_EXPERT, D_MODEL), jnp.float32)).astype(jnp.bfloat16)
    b_down = 0.5 * jax.random.normal(key_list[8], (EXPERTS, D_MODEL), jnp.float32)
    return {'hidden': hidden, 'grad_out': grad_out, 'w_router': w_router, 'b_router': b_router, 'expert_ids': expert_ids, 'slot_ids': slot_ids, 'w_gate_up': w_gate_up, 'b_gate_up': b_gate_up, 'w_down': w_down, 'b_down': b_down}


def swiglu(pre_act):
    col_pairs = pre_act.reshape(pre_act.shape[:-1] + (pre_act.shape[-1] // 2, 2))
    gate_in = jnp.minimum(col_pairs[..., 0], SWIGLU_LIMIT)
    up_in = jnp.clip(col_pairs[..., 1], -SWIGLU_LIMIT, SWIGLU_LIMIT)
    return gate_in * jax.nn.sigmoid(SWIGLU_ALPHA * gate_in) * (up_in + 1.0)


def reference(hidden, grad_out, w_router, b_router, expert_ids, slot_ids, w_gate_up, b_gate_up, w_down, b_down):
    buf_total = EXPERTS * ROWS_EXPERT
    copy_count = TOKENS * TOP_K
    src_dev = (jnp.arange(TOKENS, dtype=jnp.int32) // TOKENS_DEV)[:, None]
    dest_row = jnp.where(slot_ids >= 0, expert_ids * ROWS_EXPERT + src_dev * CAPACITY + slot_ids, buf_total)
    src_copy = jnp.full((buf_total + 1,), copy_count, jnp.int32).at[dest_row.reshape(-1)].set(jnp.arange(copy_count, dtype=jnp.int32))[:buf_total].reshape(EXPERTS, ROWS_EXPERT)
    logits = jnp.dot(hidden, w_router, preferred_element_type=jnp.float32) + b_router
    gate_w = jax.nn.softmax(jnp.take_along_axis(logits, expert_ids, axis=1), axis=-1)
    flat_gate = gate_w.reshape(-1)

    def expert_forward(expert_args):
        w_gu, b_gu, w_dn, b_dn, src_rows = expert_args
        x_rows = jnp.take(hidden, src_rows // TOP_K, axis=0, mode='fill', fill_value=0)
        pre_act = jnp.dot(x_rows, w_gu, preferred_element_type=jnp.float32) + b_gu
        act_bf = swiglu(pre_act).astype(jnp.bfloat16)
        return (jnp.dot(act_bf, w_dn, preferred_element_type=jnp.float32) + b_dn).astype(jnp.bfloat16)

    y_flat = lax.map(expert_forward, (w_gate_up, b_gate_up, w_down, b_down, src_copy)).reshape(buf_total, D_MODEL)

    def token_forward(block_args):
        gate_blk, dest_blk, grad_blk = block_args
        y_blk = jnp.take(y_flat, dest_blk, axis=0, mode='fill', fill_value=0).astype(jnp.float32)
        out_blk = jnp.sum(gate_blk[:, :, None] * y_blk, axis=1).astype(jnp.bfloat16)
        return out_blk, jnp.einsum('td,tkd->tk', grad_blk.astype(jnp.float32), y_blk)

    dev_shape = (EP_DEVICES, TOKENS_DEV)
    block_out, gate_grad = lax.map(token_forward, (gate_w.reshape(dev_shape + (TOP_K,)), dest_row.reshape(dev_shape + (TOP_K,)), grad_out.reshape(dev_shape + (D_MODEL,))))
    block_out = block_out.reshape(TOKENS, D_MODEL)
    gate_grad = gate_grad.reshape(TOKENS, TOP_K)
    sel_grad = gate_w * (gate_grad - jnp.sum(gate_w * gate_grad, axis=1, keepdims=True))
    logit_grad = jnp.zeros((TOKENS, EXPERTS), jnp.float32).at[jnp.arange(TOKENS)[:, None], expert_ids].add(sel_grad).astype(jnp.bfloat16)

    def expert_backward(expert_args):
        w_gu, b_gu, w_dn, src_rows = expert_args
        tok_rows = src_rows // TOP_K
        x_rows = jnp.take(hidden, tok_rows, axis=0, mode='fill', fill_value=0)
        pre_act = jnp.dot(x_rows, w_gu, preferred_element_type=jnp.float32) + b_gu
        act_val, act_vjp = jax.vjp(swiglu, pre_act)
        act_bf = act_val.astype(jnp.bfloat16)
        row_gate = jnp.take(flat_gate, src_rows, axis=0, mode='fill', fill_value=0)
        row_grad = jnp.take(grad_out, tok_rows, axis=0, mode='fill', fill_value=0).astype(jnp.float32)
        q_rows = (row_gate[:, None] * row_grad).astype(jnp.bfloat16)
        grad_b_dn = jnp.sum(q_rows.astype(jnp.float32), axis=0)
        grad_w_dn = jnp.dot(act_bf.T, q_rows, preferred_element_type=jnp.float32)
        act_grad = jnp.dot(q_rows, w_dn.T, preferred_element_type=jnp.float32)
        pre_grad = act_vjp(act_grad)[0].astype(jnp.bfloat16)
        grad_b_gu = jnp.sum(pre_grad.astype(jnp.float32), axis=0)
        grad_w_gu = jnp.dot(x_rows.T, pre_grad, preferred_element_type=jnp.float32)
        p_rows = jnp.dot(pre_grad, w_gu.T, preferred_element_type=jnp.float32).astype(jnp.bfloat16)
        return grad_w_gu, grad_b_gu, grad_w_dn, grad_b_dn, p_rows

    grad_w_gate_up, grad_b_gate_up, grad_w_down, grad_b_down, p_rows = lax.map(expert_backward, (w_gate_up, b_gate_up, w_down, src_copy))
    p_flat = p_rows.reshape(buf_total, D_MODEL)

    def token_backward(block_args):
        dest_blk, logit_blk = block_args
        p_blk = jnp.take(p_flat, dest_blk, axis=0, mode='fill', fill_value=0).astype(jnp.float32)
        router_dx = jnp.dot(logit_blk, w_router.T, preferred_element_type=jnp.float32)
        return (jnp.sum(p_blk, axis=1) + router_dx).astype(jnp.bfloat16)

    grad_hidden = lax.map(token_backward, (dest_row.reshape(dev_shape + (TOP_K,)), logit_grad.reshape(dev_shape + (EXPERTS,)))).reshape(TOKENS, D_MODEL)
    grad_w_router = jnp.dot(hidden.T, logit_grad, preferred_element_type=jnp.float32)
    grad_b_router = jnp.sum(logit_grad.astype(jnp.float32), axis=0)
    return (block_out, grad_hidden, grad_w_router, grad_b_router, grad_w_gate_up, grad_b_gate_up, grad_w_down, grad_b_down)
```

```python
import functools
import jax
import jax.numpy as jnp
from jax import lax
from jax.experimental import pallas as pl
from jax.experimental.pallas import tpu as pltpu
from jax.sharding import PartitionSpec as P

SWIGLU_LIMIT = 7.0
SWIGLU_ALPHA = 1.702
TILE = 512
F32 = jnp.float32
BF16 = jnp.bfloat16


def dot(a, b, ca, cb):
    return lax.dot_general(a, b, (((ca,), (cb,)), ((), ())), preferred_element_type=F32)


def expert_kernel(tile, lane0, has_acc, has_grad, *refs):
    it = iter(refs)
    x_ref, dy_ref, gate_ref, w_ref, b_ref = (next(it) for _ in range(5))
    acc_refs = [next(it) for _ in range(2)] if has_acc else []
    gin_ref = next(it) if has_grad else None
    out_ref, dx_ref, r_ref, grad_ref = (next(it) for _ in range(4))
    acc_sem = next(it) if has_acc else None
    gbuf_ref, grad_sem = (next(it), next(it)) if has_grad else (None, None)
    expert = pl.program_id(0)
    tokens, d_model = x_ref.shape
    ff = d_model // 2

    @pl.when(expert == 0)
    def _():
        if has_acc:
            loads = [pltpu.make_async_copy(src, dst, acc_sem.at[n]) for n, (src, dst) in enumerate(zip(acc_refs, (out_ref, dx_ref)))]
            for load in loads:
                load.start()
        r_ref[...] = jnp.zeros_like(r_ref)
        if has_grad:
            pltpu.make_async_copy(gin_ref.at[0], gbuf_ref, grad_sem).start()
        if has_acc:
            for load in loads:
                load.wait()
        else:
            out_ref[...] = jnp.zeros_like(out_ref)
            dx_ref[...] = jnp.zeros_like(dx_ref)

    if has_grad:
        pltpu.make_async_copy(gin_ref.at[expert], gbuf_ref, grad_sem).wait()
        grad_ref[0] = gbuf_ref[...]

        @pl.when(expert + 1 < pl.num_programs(0))
        def _():
            pltpu.make_async_copy(gin_ref.at[expert + 1], gbuf_ref, grad_sem).start()
    else:
        grad_ref[...] = jnp.zeros_like(grad_ref)

    def body(i, carry):
        rows = pl.ds(pl.multiple_of(i * tile, tile), tile)
        x = x_ref[rows, :]
        dy = dy_ref[rows, :]
        gates = gate_ref[rows, :]
        lane = lax.broadcasted_iota(jnp.int32, gates.shape, 1)
        here = lane == expert + lane0
        w = jnp.sum(jnp.where(here, gates, 0.0), axis=1, keepdims=True)
        dyf = dy.astype(F32)
        q = (w * dyf).astype(BF16)
        hg = dot(x, w_ref[0, :d_model, :ff], 1, 0) + b_ref[0, 0:1, :ff]
        hu = dot(x, w_ref[0, :d_model, ff:], 1, 0) + b_ref[0, 0:1, ff:]
        g = jnp.minimum(hg, SWIGLU_LIMIT)
        u = jnp.clip(hu, -SWIGLU_LIMIT, SWIGLU_LIMIT)
        u1 = u + 1.0
        s = 1.0 / (1.0 + jnp.exp(-SWIGLU_ALPHA * g))
        gs = g * s
        act = (gs * u1).astype(BF16)
        da = dot(q, w_ref[0, d_model:, :], 1, 1)
        y = (dot(act, w_ref[0, d_model:, :], 1, 0) + b_ref[0, 1:2, :]).astype(BF16).astype(F32)
        r = jnp.sum(y * dyf, axis=1, keepdims=True)
        r_ref[rows, :] = jnp.where(here, r, r_ref[rows, :])
        out_ref[rows, :] += w * y
        g_pass = jnp.where(hg < SWIGLU_LIMIT, 1.0, jnp.where(hg == SWIGLU_LIMIT, 0.5, 0.0))
        mag = jnp.abs(hu)
        u_pass = jnp.where(mag < SWIGLU_LIMIT, 1.0, jnp.where(mag == SWIGLU_LIMIT, 0.5, 0.0))
        dg = (da * u1 * (s + SWIGLU_ALPHA * gs * (1.0 - s)) * g_pass).astype(BF16)
        du = (da * gs * u_pass).astype(BF16)
        p = dot(dg, w_ref[0, :d_model, :ff], 1, 1) + dot(du, w_ref[0, :d_model, ff:], 1, 1)
        dx_ref[rows, :] += p.astype(BF16).astype(F32)
        grad_ref[0, :d_model, :ff] += dot(x, dg, 0, 0)
        grad_ref[0, :d_model, ff:] += dot(x, du, 0, 0)
        grad_ref[0, d_model:d_model + ff, :] += dot(act, q, 0, 0)
        row = d_model + ff
        grad_ref[0, row:row + 1, :ff] += jnp.sum(dg.astype(F32), axis=0, keepdims=True)
        grad_ref[0, row:row + 1, ff:] += jnp.sum(du.astype(F32), axis=0, keepdims=True)
        grad_ref[0, row + 1:row + 2, :] += jnp.sum(q.astype(F32), axis=0, keepdims=True)
        return carry

    lax.fori_loop(0, tokens // tile, body, 0)


def run_experts(lane0, x, dy, gates, weights, bias, acc=None, grad_in=None):
    tokens, d_model = x.shape
    experts, w_rows, _ = weights.shape
    g_rows = w_rows + 8
    once = lambda e: (0, 0)
    per = lambda e: (e, 0, 0)
    keep = pl.Buffered(1)
    full = lambda a: pl.BlockSpec(a.shape, once, pipeline_mode=keep)
    args = [x, dy, gates, weights, bias]
    specs = [full(x), full(dy), full(gates), pl.BlockSpec((1, w_rows, d_model), per), pl.BlockSpec((1, 2, d_model), per)]
    scratch = []
    if acc is not None:
        args += list(acc)
        specs += [pl.BlockSpec(memory_space=pl.ANY)] * 2
        scratch.append(pltpu.SemaphoreType.DMA((2,)))
    if grad_in is not None:
        args.append(grad_in)
        specs.append(pl.BlockSpec(memory_space=pl.ANY))
        scratch += [pltpu.VMEM((g_rows, d_model), F32), pltpu.SemaphoreType.DMA]
    tok_f32 = jax.ShapeDtypeStruct((tokens, d_model), F32)
    out_shape = [tok_f32, tok_f32, jax.ShapeDtypeStruct(gates.shape, F32), jax.ShapeDtypeStruct((experts, g_rows, d_model), F32)]
    out_specs = [pl.BlockSpec((tokens, d_model), once, pipeline_mode=keep)] * 2 + [pl.BlockSpec(gates.shape, once, pipeline_mode=keep), pl.BlockSpec((1, g_rows, d_model), per)]
    flops = 2 * experts * tokens * d_model * d_model * 9 // 2
    return pl.pallas_call(
        functools.partial(expert_kernel, min(TILE, tokens), lane0, acc is not None, grad_in is not None),
        grid=(experts,), in_specs=specs, out_specs=out_specs, out_shape=out_shape, scratch_shapes=scratch,
        compiler_params=pltpu.CompilerParams(dimension_semantics=("arbitrary",), vmem_limit_bytes=67043328),
        cost_estimate=pl.CostEstimate(flops=flops, bytes_accessed=experts * (w_rows * 2 + g_rows * 4) * d_model + tokens * d_model * 20, transcendentals=0),
        name="experts",
    )(*args)


def solution(mesh):
    ep_size = mesh.shape['ep']
    group = ep_size // 2
    groups = [list(range(group)), list(range(group, ep_size))]
    swap = [(i, (i + group) % ep_size) for i in range(ep_size)]

    def gather(a):
        return lax.all_gather(a, 'ep', axis=0, tiled=True, axis_index_groups=groups)

    def scatter(a):
        return lax.psum_scatter(a, 'ep', scatter_dimension=0, tiled=True, axis_index_groups=groups)

    def exchange(a):
        return lax.ppermute(a, 'ep', swap)

    def local_block(hidden, grad_out, w_router, b_router, expert_ids, slot_ids, w_gate_up, b_gate_up, w_down, b_down):
        tok, d_model = hidden.shape
        top_k = expert_ids.shape[1]
        experts = w_router.shape[1]
        local = w_gate_up.shape[0]
        ff = w_down.shape[1]
        half = experts // 2
        upper = lax.axis_index('ep') >= group

        src = lax.broadcasted_iota(jnp.int32, (2 * ff, 2 * ff), 0)
        dst = lax.broadcasted_iota(jnp.int32, (2 * ff, 2 * ff), 1)
        apart = (src == 2 * (dst % ff) + dst // ff)
        w_cat = [jnp.concatenate([jnp.dot(w_gate_up[c], apart.astype(BF16), preferred_element_type=F32).astype(BF16), w_down[c]], axis=0)[None] for c in range(local)]
        bias = jnp.stack([b_gate_up.reshape(local, ff, 2).transpose(0, 2, 1).reshape(local, 2 * ff), b_down], axis=1)
        w_all = [gather(w) for w in w_cat]
        b_all = gather(bias).reshape(group, local, 2, d_model)

        def order(a):
            return a.reshape(a.shape[:-1] + (2, group, local)).swapaxes(-1, -2).reshape(a.shape)

        def unorder(a):
            return a.reshape(a.shape[:-1] + (2, local, group)).swapaxes(-1, -2).reshape(a.shape)

        w_rt = order(w_router)
        ids = order(jnp.arange(experts, dtype=jnp.int32))
        logits = jnp.dot(hidden, w_rt, preferred_element_type=F32) + order(b_router)
        chosen = jnp.zeros((tok, experts), bool)
        kept = jnp.zeros((tok, experts), bool)
        for k in range(top_k):
            hit = expert_ids[:, k:k + 1] == ids[None, :]
            chosen = chosen | hit
            kept = kept | (hit & (slot_ids[:, k:k + 1] >= 0))
        top = jnp.max(jnp.where(chosen, logits, -jnp.inf), axis=1, keepdims=True)
        expo = jnp.where(chosen, jnp.exp(jnp.where(chosen, logits - top, 0.0)), 0.0)
        gate = expo / jnp.sum(expo, axis=1, keepdims=True)
        gate_kept = jnp.where(kept, gate, 0.0)
        lower_cols, upper_cols = gate_kept[:, :half], gate_kept[:, half:]
        pad = lambda a: jnp.pad(a, ((0, 0), (0, 128 - half)))
        g_own = pad(jnp.where(upper, upper_cols, lower_cols))
        x_far = exchange(hidden)
        dy_far = exchange(grad_out)
        g_far = exchange(pad(jnp.where(upper, lower_cols, upper_cols)))

        out_1, dx_1, r_1, gr_1 = run_experts(0, hidden, grad_out, g_own, w_all[0], b_all[:, 0])
        out_2, dx_2, r_2, gr_a = run_experts(0, x_far, dy_far, g_far, w_all[0], b_all[:, 0], grad_in=gr_1)
        part_a = scatter(gr_a)
        out_3, dx_3, r_3, gr_3 = run_experts(group, x_far, dy_far, g_far, w_all[1], b_all[:, 1], acc=(out_2, dx_2))
        r_far = exchange(r_2 + r_3)
        dx_far = exchange(dx_3)
        out_far = exchange(out_3)
        out_4, dx_4, r_4, gr_b = run_experts(group, hidden, grad_out, g_own, w_all[1], b_all[:, 1], acc=(out_1, dx_1), grad_in=gr_3)
        part_b = scatter(gr_b)

        block_out = (out_4 + out_far).astype(BF16)
        r_own = (r_1 + r_4)[:, :half]
        r_oth = r_far[:, :half]
        gate_grad = jnp.where(kept, jnp.concatenate([jnp.where(upper, r_oth, r_own), jnp.where(upper, r_own, r_oth)], axis=1), 0.0)
        sel_grad = gate * (gate_grad - jnp.sum(gate * gate_grad, axis=1, keepdims=True))
        logit_grad = sel_grad.astype(BF16)
        router_dx = jnp.einsum('te,de->td', logit_grad, w_rt, preferred_element_type=F32)
        grad_hidden = (dx_4 + dx_far + router_dx).astype(BF16)
        grad_rt = jnp.concatenate([jnp.einsum('te,td->ed', logit_grad, hidden, preferred_element_type=F32), jnp.pad(jnp.sum(logit_grad, axis=0, dtype=F32)[None], ((0, 7), (0, d_model - experts)))], axis=0)
        step = 1
        while step < ep_size:
            grad_rt = grad_rt + lax.ppermute(grad_rt, 'ep', [(i, i ^ step) for i in range(ep_size)])
            step *= 2
        grad_w_router = unorder(lax.optimization_barrier(grad_rt[:experts].T))
        grad_b_router = unorder(grad_rt[experts, :experts])

        def together(part):
            return lax.dot_general(part[0, :d_model], apart.astype(F32), (((1,), (1,)), ((), ())), precision=lax.Precision.HIGHEST, preferred_element_type=F32)

        parts = (part_a, part_b)
        row = d_model + ff
        grad_w_gate_up = jnp.stack([together(p) for p in parts])
        grad_w_down = jnp.stack([p[0, d_model:row] for p in parts])
        grad_b_gate_up = jnp.stack([p[0, row].reshape(2, ff).T.reshape(2 * ff) for p in parts])
        grad_b_down = jnp.stack([p[0, row + 1] for p in parts])
        return (block_out, grad_hidden, grad_w_router, grad_b_router, grad_w_gate_up, grad_b_gate_up, grad_w_down, grad_b_down)

    tok_spec = P('ep', None)
    in_specs = (tok_spec, tok_spec, P(None, None), P(None), tok_spec, tok_spec, P('ep', None, None), P('ep', None), P('ep', None, None), P('ep', None))
    out_specs = (tok_spec, tok_spec, P(None, None), P(None), P('ep', None, None), P('ep', None), P('ep', None, None), P('ep', None))
    return jax.shard_map(local_block, mesh=mesh, in_specs=in_specs, out_specs=out_specs, check_vma=False)
```

```python
import functools
import jax
import jax.numpy as jnp
from jax import lax
from jax.experimental import pallas as pl
from jax.experimental.pallas import tpu as pltpu
from jax.sharding import PartitionSpec as P

SWIGLU_LIMIT = 7.0
SWIGLU_ALPHA = 1.702
TILE = 512
F32 = jnp.float32
BF16 = jnp.bfloat16


def dot(a, b, ca, cb):
    return lax.dot_general(a, b, (((ca,), (cb,)), ((), ())), preferred_element_type=F32)


def expert_kernel(tile, lane0, stride, first, has_acc, has_grad, *refs):
    it = iter(refs)
    x_ref, dy_ref, gate_ref, w_ref, b_ref = (next(it) for _ in range(5))
    acc_refs = [next(it) for _ in range(2)] if has_acc else []
    gin_ref = next(it) if has_grad else None
    out_ref, dx_ref, r_ref, grad_ref = (next(it) for _ in range(4))
    acc_sem = next(it) if has_acc else None
    gbuf_ref, grad_sem = (next(it), next(it)) if has_grad else (None, None)
    expert = pl.program_id(0)
    tokens, d_model = x_ref.shape
    ff = d_model // 2

    @pl.when(expert == 0)
    def _():
        if has_acc:
            loads = [pltpu.make_async_copy(src, dst, acc_sem.at[n]) for n, (src, dst) in enumerate(zip(acc_refs, (out_ref, dx_ref)))]
            for load in loads:
                load.start()
        r_ref[...] = jnp.zeros_like(r_ref)
        if has_grad:
            pltpu.make_async_copy(gin_ref.at[first], gbuf_ref, grad_sem).start()
        if has_acc:
            for load in loads:
                load.wait()
        else:
            out_ref[...] = jnp.zeros_like(out_ref)
            dx_ref[...] = jnp.zeros_like(dx_ref)

    if has_grad:
        pltpu.make_async_copy(gin_ref.at[first + stride * expert], gbuf_ref, grad_sem).wait()
        grad_ref[0] = gbuf_ref[...]

        @pl.when(expert + 1 < pl.num_programs(0))
        def _():
            pltpu.make_async_copy(gin_ref.at[first + stride * (expert + 1)], gbuf_ref, grad_sem).start()
    else:
        grad_ref[...] = jnp.zeros_like(grad_ref)

    def body(i, carry):
        rows = pl.ds(pl.multiple_of(i * tile, tile), tile)
        x = x_ref[rows, :]
        dy = dy_ref[rows, :]
        gates = gate_ref[rows, :]
        lane = lax.broadcasted_iota(jnp.int32, gates.shape, 1)
        here = lane == lane0 + first + stride * expert
        w = jnp.sum(jnp.where(here, gates, 0.0), axis=1, keepdims=True)
        dyf = dy.astype(F32)
        q = (w * dyf).astype(BF16)
        h = dot(x, w_ref[0, :d_model, :], 1, 0) + b_ref[0, 0:1, :]
        hg, hu = h[:, :ff], h[:, ff:]
        g = jnp.minimum(hg, SWIGLU_LIMIT)
        u = jnp.clip(hu, -SWIGLU_LIMIT, SWIGLU_LIMIT)
        u1 = u + 1.0
        s = 1.0 / (1.0 + jnp.exp(-SWIGLU_ALPHA * g))
        gs = g * s
        act = (gs * u1).astype(BF16)
        da = dot(q, w_ref[0, d_model:, :], 1, 1)
        y = (dot(act, w_ref[0, d_model:, :], 1, 0) + b_ref[0, 1:2, :]).astype(BF16).astype(F32)
        r = jnp.sum(y * dyf, axis=1, keepdims=True)
        r_ref[rows, :] = jnp.where(here, r, r_ref[rows, :])
        out_ref[rows, :] += w * y
        g_pass = jnp.where(hg < SWIGLU_LIMIT, 1.0, jnp.where(hg == SWIGLU_LIMIT, 0.5, 0.0))
        mag = jnp.abs(hu)
        u_pass = jnp.where(mag < SWIGLU_LIMIT, 1.0, jnp.where(mag == SWIGLU_LIMIT, 0.5, 0.0))
        dg = (da * u1 * (s + SWIGLU_ALPHA * gs * (1.0 - s)) * g_pass).astype(BF16)
        du = (da * gs * u_pass).astype(BF16)
        dh = jnp.concatenate([dg, du], axis=1)
        p = dot(dh, w_ref[0, :d_model, :], 1, 1)
        dx_ref[rows, :] += p.astype(BF16).astype(F32)
        grad_ref[0, :d_model, :] += dot(x, dh, 0, 0)
        grad_ref[0, d_model:d_model + ff, :] += dot(act, q, 0, 0)
        row = d_model + ff
        grad_ref[0, row:row + 1, :] += jnp.sum(dh.astype(F32), axis=0, keepdims=True)
        grad_ref[0, row + 1:row + 2, :] += jnp.sum(q.astype(F32), axis=0, keepdims=True)
        return carry

    lax.fori_loop(0, tokens // tile, body, 0)


def run_experts(lane0, x, dy, gates, weights, bias, acc=None, grad_in=None, stride=1, first=0):
    tokens, d_model = x.shape
    experts, w_rows = weights.shape[0] // stride, weights.shape[1]
    g_rows = w_rows + 16
    once = lambda e: (0, 0)
    per = lambda e: (e, 0, 0)
    pick = lambda e: (first + stride * e, 0, 0)
    keep = pl.Buffered(1)
    full = lambda a: pl.BlockSpec(a.shape, once, pipeline_mode=keep)
    args = [x, dy, gates, weights, bias]
    specs = [full(x), full(dy), full(gates), pl.BlockSpec((1, w_rows, d_model), pick), pl.BlockSpec((1, 2, d_model), pick)]
    scratch = []
    if acc is not None:
        args += list(acc)
        specs += [pl.BlockSpec(memory_space=pl.ANY)] * 2
        scratch.append(pltpu.SemaphoreType.DMA((2,)))
    if grad_in is not None:
        args.append(grad_in)
        specs.append(pl.BlockSpec(memory_space=pl.ANY))
        scratch += [pltpu.VMEM((g_rows, d_model), F32), pltpu.SemaphoreType.DMA]
    tok_f32 = jax.ShapeDtypeStruct((tokens, d_model), F32)
    out_shape = [tok_f32, tok_f32, jax.ShapeDtypeStruct(gates.shape, F32), jax.ShapeDtypeStruct((experts, g_rows, d_model), F32)]
    out_specs = [pl.BlockSpec((tokens, d_model), once, pipeline_mode=keep)] * 2 + [pl.BlockSpec(gates.shape, once, pipeline_mode=keep), pl.BlockSpec((1, g_rows, d_model), per)]
    flops = 2 * experts * tokens * d_model * d_model * 9 // 2
    return pl.pallas_call(
        functools.partial(expert_kernel, min(TILE, tokens), lane0, stride, first, acc is not None, grad_in is not None),
        grid=(experts,), in_specs=specs, out_specs=out_specs, out_shape=out_shape, scratch_shapes=scratch,
        compiler_params=pltpu.CompilerParams(dimension_semantics=("arbitrary",), vmem_limit_bytes=67043328),
        cost_estimate=pl.CostEstimate(flops=flops, bytes_accessed=experts * (w_rows * 2 + g_rows * 4) * d_model + tokens * d_model * 20, transcendentals=0),
        name="experts",
    )(*args)


def solution(mesh):
    ep_size = mesh.shape['ep']
    group = ep_size // 2
    groups = [list(range(group)), list(range(group, ep_size))]
    swap = [(i, (i + group) % ep_size) for i in range(ep_size)]

    def gather(a):
        return lax.all_gather(a, 'ep', axis=0, tiled=True, axis_index_groups=groups)

    def scatter(a):
        return lax.psum_scatter(a, 'ep', scatter_dimension=0, tiled=True, axis_index_groups=groups)

    def exchange(a):
        return lax.ppermute(a, 'ep', swap)

    def local_block(hidden, grad_out, w_router, b_router, expert_ids, slot_ids, w_gate_up, b_gate_up, w_down, b_down):
        tok, d_model = hidden.shape
        top_k = expert_ids.shape[1]
        experts = w_router.shape[1]
        local = w_gate_up.shape[0]
        ff = w_down.shape[1]
        half = experts // 2
        upper = lax.axis_index('ep') >= group

        src = lax.broadcasted_iota(jnp.int32, (2 * ff, 2 * ff), 0)
        dst = lax.broadcasted_iota(jnp.int32, (2 * ff, 2 * ff), 1)
        apart = (src == 2 * (dst % ff) + dst // ff)
        w_cat = [jnp.concatenate([jnp.dot(w_gate_up[c], apart.astype(BF16), preferred_element_type=F32).astype(BF16), w_down[c]], axis=0)[None] for c in range(local)]
        bias = jnp.stack([b_gate_up.reshape(local, ff, 2).transpose(0, 2, 1).reshape(local, 2 * ff), b_down], axis=1)
        w_all = [gather(w) for w in w_cat]
        b_all = gather(bias).reshape(group, local, 2, d_model)

        def order(a):
            return a.reshape(a.shape[:-1] + (2, group, local)).swapaxes(-1, -2).reshape(a.shape)

        def unorder(a):
            return a.reshape(a.shape[:-1] + (2, local, group)).swapaxes(-1, -2).reshape(a.shape)

        w_rt = order(w_router)
        ids = order(jnp.arange(experts, dtype=jnp.int32))
        logits = jnp.dot(hidden, w_rt, preferred_element_type=F32) + order(b_router)
        chosen = jnp.zeros((tok, experts), bool)
        kept = jnp.zeros((tok, experts), bool)
        for k in range(top_k):
            hit = expert_ids[:, k:k + 1] == ids[None, :]
            chosen = chosen | hit
            kept = kept | (hit & (slot_ids[:, k:k + 1] >= 0))
        top = jnp.max(jnp.where(chosen, logits, -jnp.inf), axis=1, keepdims=True)
        expo = jnp.where(chosen, jnp.exp(jnp.where(chosen, logits - top, 0.0)), 0.0)
        gate = expo / jnp.sum(expo, axis=1, keepdims=True)
        gate_kept = jnp.where(kept, gate, 0.0)
        lower_cols, upper_cols = gate_kept[:, :half], gate_kept[:, half:]
        pad = lambda a: jnp.pad(a, ((0, 0), (0, 128 - half)))
        g_own = pad(jnp.where(upper, upper_cols, lower_cols))
        x_far = exchange(hidden)
        dy_far = exchange(grad_out)
        g_far = exchange(pad(jnp.where(upper, lower_cols, upper_cols)))

        out_1, dx_1, r_1, gr_1 = run_experts(0, hidden, grad_out, g_own, w_all[0], b_all[:, 0])
        out_2, dx_2, r_2, gr_a = run_experts(0, x_far, dy_far, g_far, w_all[0], b_all[:, 0], grad_in=gr_1)
        part_a = scatter(gr_a)
        out_3, dx_3, r_3, gr_3 = run_experts(group, x_far, dy_far, g_far, w_all[1], b_all[:, 1], acc=(out_2, dx_2))
        r_far = exchange(r_2 + r_3)
        dx_far = exchange(dx_3)
        out_far = exchange(out_3)
        out_4, dx_4, r_4, gr_b = run_experts(group, hidden, grad_out, g_own, w_all[1], b_all[:, 1], acc=(out_1, dx_1), grad_in=gr_3, stride=2, first=0)
        half_0 = scatter(gr_b.reshape(-1, d_model))
        out_5, dx_5, r_5, gr_c = run_experts(group, hidden, grad_out, g_own, w_all[1], b_all[:, 1], acc=(out_4, dx_4), grad_in=gr_3, stride=2, first=1)
        half_1 = scatter(gr_c.reshape(-1, d_model))
        odd = lax.axis_index('ep') % 2 == 1
        got = lax.ppermute(jnp.where(odd, half_0, half_1), 'ep', [(i, i ^ 1) for i in range(ep_size)])
        part_b = jnp.concatenate([jnp.where(odd, got, half_0), jnp.where(odd, half_1, got)], axis=0)[None]

        block_out = (out_5 + out_far).astype(BF16)
        r_own = (r_1 + r_4 + r_5)[:, :half]
        r_oth = r_far[:, :half]
        gate_grad = jnp.where(kept, jnp.concatenate([jnp.where(upper, r_oth, r_own), jnp.where(upper, r_own, r_oth)], axis=1), 0.0)
        sel_grad = gate * (gate_grad - jnp.sum(gate * gate_grad, axis=1, keepdims=True))
        logit_grad = sel_grad.astype(BF16)
        router_dx = jnp.einsum('te,de->td', logit_grad, w_rt, preferred_element_type=F32)
        grad_hidden = (dx_5 + dx_far + router_dx).astype(BF16)
        grad_rt = jnp.concatenate([jnp.einsum('te,td->ed', logit_grad, hidden, preferred_element_type=F32), jnp.pad(jnp.sum(logit_grad, axis=0, dtype=F32)[None], ((0, 7), (0, d_model - experts)))], axis=0)
        step = 1
        while step < ep_size:
            grad_rt = grad_rt + lax.ppermute(grad_rt, 'ep', [(i, i ^ step) for i in range(ep_size)])
            step *= 2
        grad_w_router = unorder(lax.optimization_barrier(grad_rt[:experts].T))
        grad_b_router = unorder(grad_rt[experts, :experts])

        def together(part):
            return lax.dot_general(part[0, :d_model], apart.astype(F32), (((1,), (1,)), ((), ())), precision=lax.Precision.HIGHEST, preferred_element_type=F32)

        parts = (part_a, part_b)
        row = d_model + ff
        grad_w_gate_up = jnp.stack([together(p) for p in parts])
        grad_w_down = jnp.stack([p[0, d_model:row] for p in parts])
        grad_b_gate_up = jnp.stack([p[0, row].reshape(2, ff).T.reshape(2 * ff) for p in parts])
        grad_b_down = jnp.stack([p[0, row + 1] for p in parts])
        return (block_out, grad_hidden, grad_w_router, grad_b_router, grad_w_gate_up, grad_b_gate_up, grad_w_down, grad_b_down)

    tok_spec = P('ep', None)
    in_specs = (tok_spec, tok_spec, P(None, None), P(None), tok_spec, tok_spec, P('ep', None, None), P('ep', None), P('ep', None, None), P('ep', None))
    out_specs = (tok_spec, tok_spec, P(None, None), P(None), P('ep', None, None), P('ep', None), P('ep', None, None), P('ep', None))
    return jax.shard_map(local_block, mesh=mesh, in_specs=in_specs, out_specs=out_specs, check_vma=False)
```
